32 devices in a mesh: dp: 8 (over z, x), hyper: 4 (over y, core).
Axes of the slice: x: 2, y: 2, z: 4, core: 2. Of those that a mesh axis runs over, the one named last changes fastest.
Arguments:
- inputs: bfloat16 [64, 64, 128], P(('dp', 'hyper')), may hold values from -64 to 64
- labels: int32 [64, 64], P(('dp', 'hyper')), may hold values from 0 to 255
- client_ids: int32 [64], P(('dp', 'hyper')), may hold values from 0 to 63
- ext_weight: bfloat16 [128, 4096], replicated, may hold values from -0.5 to 0.5
- ext_bias: bfloat16 [4096], replicated, may hold values from -3 to 3
- embeddings: bfloat16 [64, 128], replicated, may hold values from -1.5 to 1.5
- hyper_in: bfloat16 [128, 50], replicated, may hold values from -2.09375 to 2.09375
- hyper_bias: float32 [50], replicated, may hold values from -3 to 3
- hyper_out: bfloat16 [4096, 50, 256], P('hyper'), may hold values from -0.1796875 to 0.1796875
Outputs:
- grad_ext_weight: float32 [128, 4096], replicated
- grad_ext_bias: float32 [4096], replicated
- grad_embeddings: float32 [64, 128], replicated
- grad_hyper_in: float32 [128, 50], replicated
- grad_hyper_bias: float32 [50], replicated
- grad_hyper_out: float32 [4096, 50, 256], P(('hyper', 'dp'))
The draws below stay inside these ranges and needn't reach their ends.
Inputs may be any that keep to these rules, and one draw needn't show every extreme that they name: `client_ids`: A client may hold several slots or none.
All inputs are finite; a program needn't handle non-finite values.
Results may differ from the reference program's by a relative error of at most 0.014.
The reference program's roundings to bfloat16 on the way count: a program that leaves them out, or rounds other values in their place, can miss the bound.
Values may be sent and summed in bfloat16 or wider, within the bound.
A program may use at most 192 MiB of HBM per device.

```python
import jax
import jax.numpy as jnp
from jax import lax

D = 4096
C = 256
DIN = 128
HH = 50
E = 128
CD = 2
R = 64
SLOTS = 64
NCL = 64
N_DP = 8
N_HYPER = 4


def draw_inputs(key, part):
    values = jax.random.normal(key, (SLOTS, R, DIN), jnp.float32)
    values = jnp.clip(values, -6.0, 6.0)
    return jnp.clip(values, -64.0, 64.0).astype(jnp.bfloat16)


def with_ends(result, key, low, high):
    shape = result.shape
    place = [jax.random.randint(jax.random.fold_in(key, axis), (), 0, shape[axis]) for axis in range(len(shape))]
    result = result.at[tuple(place)].set(low)
    longest = shape.index(max(shape))
    place[longest] = (place[longest] + 1) % shape[longest]
    return result.at[tuple(place)].set(high)


def block_scale(rng, dims, cuts, smallest, high):
    loudness = 1.0
    for axis_at, shards_of in cuts:
        draws = jax.random.uniform(jax.random.fold_in(jax.random.fold_in(rng, 6), axis_at), (shards_of,), jnp.float32, smallest / len(cuts), high / len(cuts))
        loudness = loudness * jnp.repeat(jnp.exp(draws), dims[axis_at] // shards_of).reshape((-1,) + (1,) * (len(dims) - 1 - axis_at))
    return loudness


def gaussian(own_key, extent, spread, bound, shards=(), kind=jnp.bfloat16):
    loudness = block_scale(own_key, extent, shards, -0.22, 0.18) if shards else 1.0
    array = jax.random.normal(own_key, extent, jnp.float32) * spread * loudness
    return jnp.minimum(jnp.maximum(array, -bound), bound).astype(kind)


def setup_inputs(seed: int = 0) -> dict:
    splits = jax.random.split(jax.random.key(seed), 10)
    return {
        "inputs": draw_inputs(jax.random.fold_in(splits[9], 71), 0),
        "labels": with_ends(jax.random.randint(splits[1], (SLOTS, R), 0, C), jax.random.fold_in(splits[1], 1), 0, C - 1).astype(jnp.int32),
        "client_ids": with_ends(jax.random.randint(splits[2], (SLOTS,), 0, NCL), jax.random.fold_in(splits[2], 1), 0, NCL - 1).astype(jnp.int32),
        "ext_weight": gaussian(splits[3], (DIN, D), DIN ** -0.5, 0.5),
        "ext_bias": gaussian(splits[4], (D,), 0.5, 3.0),
        "embeddings": gaussian(splits[5], (NCL, E), 0.25, 1.5),
        "hyper_in": gaussian(splits[6], (E, HH), 0.35, 2.09375),
        "hyper_bias": gaussian(splits[7], (HH,), 0.5, 3.0, (), jnp.float32),
        "hyper_out": gaussian(splits[8], (D, HH, C), 0.03, 0.1796875, ((0, 4),)),
    }


highest = lax.Precision.HIGHEST


def silu_slope(values):
    logistic = jax.nn.sigmoid(values)
    return logistic * (1.0 + values * (1.0 - logistic))


def class_grads(logits, slot_labels, row_count):
    largest = jnp.max(logits, axis=-1, keepdims=True)
    exponent = jnp.exp(logits - largest)
    probability = exponent / jnp.sum(exponent, axis=-1, keepdims=True)
    classes = jnp.arange(logits.shape[-1], dtype=jnp.int32)
    onehot = (slot_labels[..., None] == classes).astype(jnp.float32)
    return ((probability - onehot) / row_count).astype(jnp.bfloat16)


def reference(inputs, labels, client_ids, ext_weight, ext_bias, embeddings, hyper_in, hyper_bias, hyper_out):
    group_size = N_HYPER * CD
    hyper_wide = hyper_out.astype(jnp.float32)
    hyper_in_wide = hyper_in.astype(jnp.float32)
    client_table = jnp.arange(NCL, dtype=jnp.int32)

    def one_group(totals, group_index):
        first_slot = (group_index * group_size).astype(jnp.int32)
        slot_inputs = lax.dynamic_slice_in_dim(inputs, first_slot, group_size, 0)
        slot_labels = lax.dynamic_slice_in_dim(labels, first_slot, group_size, 0)
        slot_ids = lax.dynamic_slice_in_dim(client_ids, first_slot, group_size, 0)
        flat_in = slot_inputs.reshape(group_size * R, DIN)
        preact = jnp.dot(flat_in, ext_weight, preferred_element_type=jnp.float32) + ext_bias.astype(jnp.float32)
        features = jax.nn.silu(preact).astype(jnp.bfloat16).reshape(group_size, R, D)
        picked = embeddings[slot_ids]
        hyper_preact = jnp.dot(picked, hyper_in, preferred_element_type=jnp.float32) + hyper_bias
        hidden = jax.nn.silu(hyper_preact).astype(jnp.bfloat16)
        client_heads = jnp.einsum("kh,dhc->kdc", hidden.astype(jnp.float32), hyper_wide).astype(jnp.bfloat16)
        feat_wide = features.astype(jnp.float32)
        heads_wide = client_heads.astype(jnp.float32)
        logits = jnp.einsum("krd,kdc->krc", feat_wide, heads_wide)
        dlogits = class_grads(logits, slot_labels, R)
        dlog_wide = dlogits.astype(jnp.float32)
        dheads = jnp.einsum("krd,krc->kdc", feat_wide, dlog_wide).astype(jnp.bfloat16)
        dfeatures = jnp.einsum("krc,kdc->krd", dlog_wide, heads_wide).astype(jnp.bfloat16)
        dpreact = (dfeatures.reshape(group_size * R, D).astype(jnp.float32) * silu_slope(preact)).astype(jnp.bfloat16)
        grad_weight = jnp.dot(flat_in.T, dpreact, preferred_element_type=jnp.float32)
        grad_bias = jnp.sum(dpreact.astype(jnp.float32), axis=0)
        dheads_wide = dheads.astype(jnp.float32)
        group_out = jnp.einsum("kh,kdc->dhc", hidden.astype(jnp.float32), dheads_wide)
        group_out = lax.optimization_barrier(group_out.astype(jnp.bfloat16)).astype(jnp.float32)
        dhidden = jnp.einsum("kdc,dhc->kh", dheads_wide, hyper_wide)
        hyper_dpre = dhidden * silu_slope(hyper_preact)
        grad_in = jnp.dot(picked.astype(jnp.float32).T, hyper_dpre, precision=highest)
        grad_hbias = jnp.sum(hyper_dpre, axis=0)
        select = (slot_ids[:, None] == client_table[None, :]).astype(jnp.float32)
        grad_table = jnp.dot(select.T, jnp.dot(hyper_dpre, hyper_in_wide.T, precision=highest), precision=highest)
        updated = (totals[0] + grad_weight, totals[1] + grad_bias, totals[2] + grad_table,
                   totals[3] + grad_in, totals[4] + grad_hbias, totals[5] + group_out)
        return updated, None

    initial = (jnp.zeros((DIN, D), jnp.float32), jnp.zeros((D,), jnp.float32), jnp.zeros((NCL, E), jnp.float32),
               jnp.zeros((E, HH), jnp.float32), jnp.zeros((HH,), jnp.float32), jnp.zeros((D, HH, C), jnp.float32))
    totals, unused = lax.scan(one_group, initial, jnp.arange(N_DP, dtype=jnp.int32))
    return (totals[0], totals[1], totals[2], totals[3], totals[4], totals[5])
```

```python
import jax
import jax.numpy as jnp
from jax import lax
from jax.sharding import PartitionSpec as P

highest = lax.Precision.HIGHEST
f32 = jnp.float32
bf16 = jnp.bfloat16


def silu_slope(values):
    logistic = jax.nn.sigmoid(values)
    return logistic * (1.0 + values * (1.0 - logistic))


def class_grads(logits, slot_labels, row_count):
    largest = jnp.max(logits, axis=-1, keepdims=True)
    exponent = jnp.exp(logits - largest)
    probability = exponent / jnp.sum(exponent, axis=-1, keepdims=True)
    classes = jnp.arange(logits.shape[-1], dtype=jnp.int32)
    onehot = (slot_labels[..., None] == classes).astype(f32)
    return ((probability - onehot) / row_count).astype(bf16)


def local(
    inputs, labels, client_ids, ext_weight, ext_bias, embeddings, hyper_in, hyper_bias, hyper_out
):
    everyone = ("dp", "hyper")
    n_dp, n_hyper = lax.axis_size("dp"), lax.axis_size("hyper")
    i, j = lax.axis_index("dp"), lax.axis_index("hyper")
    own, rows, width_in = inputs.shape
    wide = hyper_out.shape[0]
    narrow = wide // n_dp
    group = own * n_hyper
    slots = group * n_dp
    classes = hyper_out.shape[2]

    ids = lax.all_gather(client_ids, everyone, axis=0, tiled=True)
    in_group = lax.all_gather(inputs, "hyper", axis=0, tiled=True)
    in_all = lax.all_gather(in_group, "dp", axis=0, tiled=True)
    select = (ids[:, None] == jnp.arange(embeddings.shape[0], dtype=jnp.int32)[None, :])
    picked = jnp.dot(select.astype(bf16), embeddings, preferred_element_type=f32).astype(bf16)
    hyper_preact = jnp.dot(picked, hyper_in, preferred_element_type=f32) + hyper_bias
    hidden = jax.nn.silu(hyper_preact).astype(bf16)

    w_wide = lax.dynamic_slice_in_dim(ext_weight, j * wide, wide, 1)
    b_wide = lax.dynamic_slice_in_dim(ext_bias, j * wide, wide, 0).astype(f32)
    preact = jnp.dot(in_group.reshape(group * rows, width_in), w_wide, preferred_element_type=f32)
    features = jax.nn.silu(preact + b_wide).astype(bf16).reshape(group, rows, wide)
    hidden_group = lax.dynamic_slice_in_dim(hidden, i * group, group, 0)
    heads = jnp.einsum("kh,dhc->kdc", hidden_group, hyper_out, preferred_element_type=f32)
    part = jnp.einsum("krd,kdc->krc", features, heads.astype(bf16), preferred_element_type=f32)
    parts = lax.all_to_all(
        part.reshape(n_hyper, own * rows, classes), "hyper", split_axis=0, concat_axis=0
    )
    logits = jnp.sum(parts, axis=0).reshape(own, rows, classes)
    dlogits = class_grads(logits, labels, rows)
    dl_all = lax.all_gather(dlogits, everyone, axis=0, tiled=True)

    start = (j * n_dp + i) * narrow
    w = lax.dynamic_slice_in_dim(ext_weight, start, narrow, 1)
    b = lax.dynamic_slice_in_dim(ext_bias, start, narrow, 0).astype(f32)
    out_rows = lax.dynamic_slice_in_dim(hyper_out, i * narrow, narrow, 0)
    flat = in_all.reshape(slots * rows, width_in)
    preact = jnp.dot(flat, w, preferred_element_type=f32) + b
    features = jax.nn.silu(preact).astype(bf16).reshape(slots, rows, narrow)
    heads = jnp.einsum("kh,dhc->kdc", hidden, out_rows, preferred_element_type=f32).astype(bf16)
    dheads = jnp.einsum("krd,krc->kdc", features, dl_all, preferred_element_type=f32).astype(bf16)
    dfeatures = jnp.einsum("krc,kdc->krd", dl_all, heads, preferred_element_type=f32).astype(bf16)
    dpreact = (
        dfeatures.reshape(slots * rows, narrow).astype(f32) * silu_slope(preact)
    ).astype(bf16)
    grad_weight = jnp.dot(flat.T, dpreact, preferred_element_type=f32)
    grad_bias = jnp.sum(dpreact.astype(f32), axis=0)
    grad_out = jnp.einsum("kh,kdc->dhc", hidden, dheads, preferred_element_type=f32)
    dhidden = jnp.einsum("kdc,dhc->kh", dheads, out_rows, preferred_element_type=f32)
    dhidden = lax.psum(dhidden, everyone)
    hyper_dpre = dhidden * silu_slope(hyper_preact)
    grad_in = jnp.dot(picked.astype(f32).T, hyper_dpre, precision=highest)
    grad_hbias = jnp.sum(hyper_dpre, axis=0)
    back_rows = jnp.dot(hyper_dpre, hyper_in.astype(f32).T, precision=highest)
    grad_table = jnp.dot(select.astype(f32).T, back_rows, precision=highest)
    both = jnp.concatenate([grad_weight, grad_bias[None]], axis=0)
    both = lax.all_gather(both, ("hyper", "dp"), axis=1, tiled=True)
    return (both[:-1], both[-1], grad_table, grad_in, grad_hbias, grad_out)


def solution(mesh):
    placed = (
        P(("dp", "hyper"), None, None),
        P(("dp", "hyper"), None),
        P(("dp", "hyper")),
        P(),
        P(),
        P(),
        P(),
        P(),
        P("hyper", None, None),
    )
    return jax.shard_map(
        local,
        mesh=mesh,
        in_specs=placed,
        out_specs=(P(), P(), P(), P(), P(), P(("hyper", "dp"), None, None)),
        check_vma=False,
    )
```

```python
import jax
import jax.numpy as jnp
from jax import lax
from jax.sharding import PartitionSpec as P

highest = lax.Precision.HIGHEST
f32 = jnp.float32
bf16 = jnp.bfloat16


def silu_slope(values):
    logistic = jax.nn.sigmoid(values)
    return logistic * (1.0 + values * (1.0 - logistic))


def class_grads(logits, slot_labels, row_count):
    largest = jnp.max(logits, axis=-1, keepdims=True)
    exponent = jnp.exp(logits - largest)
    probability = exponent / jnp.sum(exponent, axis=-1, keepdims=True)
    classes = jnp.arange(logits.shape[-1], dtype=jnp.int32)
    onehot = (slot_labels[..., None] == classes).astype(f32)
    return ((probability - onehot) / row_count).astype(bf16)


def local(
    inputs, labels, client_ids, ext_weight, ext_bias, embeddings, hyper_in, hyper_bias, hyper_out
):
    everyone = ("dp", "hyper")
    n_dp, n_hyper = lax.axis_size("dp"), lax.axis_size("hyper")
    i, j = lax.axis_index("dp"), lax.axis_index("hyper")
    own, rows, width_in = inputs.shape
    wide = hyper_out.shape[0]
    narrow = wide // n_dp
    group = own * n_hyper
    slots = group * n_dp
    classes = hyper_out.shape[2]

    parts_of_ids = jnp.stack([client_ids // 256, client_ids % 256]).astype(bf16)
    flat_own = inputs.reshape(own * rows, width_in)
    packed = jnp.concatenate([flat_own, jnp.pad(parts_of_ids, ((0, 14), (0, width_in - own)))])
    from_group = lax.all_gather(packed, "hyper", axis=0)
    from_all = lax.all_gather(from_group, "dp", axis=0)
    table = jnp.arange(embeddings.shape[0], dtype=jnp.int32)

    def hypernet(gathered):
        gathered = gathered.reshape(-1, own * rows + 16, width_in)
        halves = gathered[:, own * rows : own * rows + 2, :own].astype(f32).astype(jnp.int32)
        ids = (halves[:, 0] * 256 + halves[:, 1]).reshape(-1)
        select = ids[:, None] == table[None, :]
        picked = jnp.dot(select.astype(bf16), embeddings, preferred_element_type=f32).astype(bf16)
        hyper_preact = jnp.dot(picked, hyper_in, preferred_element_type=f32) + hyper_bias
        hidden = jax.nn.silu(hyper_preact).astype(bf16)
        return select, picked, hyper_preact, hidden, gathered[:, : own * rows]

    hidden_group, in_group = hypernet(from_group)[3:]

    w_wide = lax.dynamic_slice_in_dim(ext_weight, j * wide, wide, 1)
    b_wide = lax.dynamic_slice_in_dim(ext_bias, j * wide, wide, 0).astype(f32)
    preact = jnp.dot(in_group.reshape(group * rows, width_in), w_wide, preferred_element_type=f32)
    features = jax.nn.silu(preact + b_wide).astype(bf16).reshape(group, rows, wide)
    heads = jnp.einsum("kh,dhc->kdc", hidden_group, hyper_out, preferred_element_type=f32)
    part = jnp.einsum("krd,kdc->krc", features, heads.astype(bf16), preferred_element_type=f32)
    parts = lax.all_to_all(
        part.reshape(n_hyper, own * rows, classes), "hyper", split_axis=0, concat_axis=0
    )
    logits = jnp.sum(parts, axis=0).reshape(own, rows, classes)
    dlogits = class_grads(logits, labels, rows)
    dlogits, from_all = lax.optimization_barrier((dlogits, from_all))
    select, picked, hyper_preact, hidden, in_all = hypernet(from_all)
    dl_all = lax.all_gather(dlogits, everyone, axis=0, tiled=True)

    start = (j * n_dp + i) * narrow
    w = lax.dynamic_slice_in_dim(ext_weight, start, narrow, 1)
    b = lax.dynamic_slice_in_dim(ext_bias, start, narrow, 0).astype(f32)
    out_rows = lax.dynamic_slice_in_dim(hyper_out, i * narrow, narrow, 0)
    out_rows = lax.optimization_barrier(out_rows)
    flat = in_all.reshape(slots * rows, width_in)
    preact = jnp.dot(flat, w, preferred_element_type=f32) + b
    features = jax.nn.silu(preact).astype(bf16).reshape(slots, rows, narrow)
    heads = jnp.einsum("kh,dhc->kdc", hidden, out_rows, preferred_element_type=f32).astype(bf16)
    dheads = jnp.einsum("krd,krc->kdc", features, dl_all, preferred_element_type=f32).astype(bf16)
    dfeatures = jnp.einsum("krc,kdc->krd", dl_all, heads, preferred_element_type=f32).astype(bf16)
    dpreact = (
        dfeatures.reshape(slots * rows, narrow).astype(f32) * silu_slope(preact)
    ).astype(bf16)
    grad_weight = jnp.dot(flat.T, dpreact, preferred_element_type=f32)
    grad_bias = jnp.sum(dpreact.astype(f32), axis=0)
    grad_out = jnp.einsum("kh,kdc->dhc", hidden, dheads, preferred_element_type=f32)
    dhidden = jnp.einsum("kdc,dhc->kh", dheads, out_rows, preferred_element_type=f32)
    bias_rows = jnp.zeros((n_hyper * n_dp, narrow), f32)
    bias_rows = lax.dynamic_update_slice_in_dim(bias_rows, grad_bias[None], j * n_dp + i, 0)
    dhidden, bias_rows = lax.psum((dhidden, bias_rows), everyone)
    hyper_dpre = dhidden * silu_slope(hyper_preact)
    grad_in = jnp.dot(picked.astype(f32).T, hyper_dpre, precision=highest)
    grad_hbias = jnp.sum(hyper_dpre, axis=0)
    back_rows = jnp.dot(hyper_dpre, hyper_in.astype(f32).T, precision=highest)
    grad_table = jnp.dot(select.astype(f32).T, back_rows, precision=highest)
    grad_weight = lax.all_gather(grad_weight, ("hyper", "dp"), axis=1, tiled=True)
    return (grad_weight, bias_rows.reshape(-1), grad_table, grad_in, grad_hbias, grad_out)


def solution(mesh):
    placed = (
        P(("dp", "hyper"), None, None),
        P(("dp", "hyper"), None),
        P(("dp", "hyper")),
        P(),
        P(),
        P(),
        P(),
        P(),
        P("hyper", None, None),
    )
    return jax.shard_map(
        local,
        mesh=mesh,
        in_specs=placed,
        out_specs=(P(), P(), P(), P(), P(), P(("hyper", "dp"), None, None)),
        check_vma=False,
    )
```
